8 devices in a mesh: dp: 2 (over z, y), sp: 4 (over x, core).
Axes of the slice: x: 2, y: 2, z: 1, core: 2. Of those that a mesh axis runs over, the one named last changes fastest.
Arguments:
- x_in: bfloat16 [64, 256, 2048], P('dp', 'sp'), parts along dimension 0
- dy_out: bfloat16 [64, 256, 2048], P('dp', 'sp'), parts along dimension 0
- w_query: bfloat16 [2048, 2048], replicated
- w_key: bfloat16 [2048, 2048], replicated
- w_value: bfloat16 [2048, 2048], replicated
- w_beta: bfloat16 [2048, 16], replicated
- conv_query: bfloat16 [4, 2048], replicated
- conv_key: bfloat16 [4, 2048], replicated
- conv_value: bfloat16 [4, 2048], replicated
- w_gate: bfloat16 [2048, 2048], replicated
- norm_weight: bfloat16 [128], replicated
- w_out: bfloat16 [2048, 2048], replicated
Outputs:
- output 1: bfloat16 [64, 256, 2048], P('dp', 'sp'), parts along dimension 0
- output 2: bfloat16 [64, 256, 2048], P('dp', 'sp'), parts along dimension 0
- output 3: float32 [4096, 2048], P('dp'), parts along dimension 0
- output 4: float32 [4096, 2048], P('dp'), parts along dimension 0
- output 5: float32 [4096, 2048], P('dp'), parts along dimension 0
- output 6: float32 [4096, 16], P('dp'), parts along dimension 0
- output 7: float32 [8, 2048], P('dp'), parts along dimension 0
- output 8: float32 [8, 2048], P('dp'), parts along dimension 0
- output 9: float32 [8, 2048], P('dp'), parts along dimension 0
- output 10: float32 [4096, 2048], P('dp'), parts along dimension 0
- output 11: float32 [256], P('dp'), parts along dimension 0
- output 12: float32 [4096, 2048], P('dp'), parts along dimension 0
There are 2 independent parts. The reference program is written for one: setup_inputs(seed, part) draws one part's arguments, and reference() takes and returns one part's arrays. A program takes and returns all parts, laid end to end along the dimension named above; an argument that names none is the same for every part.
All inputs are finite; a program needn't handle non-finite values.
Results may differ from the reference program's by a relative error of at most 0.015849.
Values are sent between devices in bfloat16 or wider.
A program may use at most 1 GiB of HBM per device.

```python
import jax
import jax.numpy as jnp
from jax import lax

BATCH_SIZE = 32
SEQ_LEN = 256
MODEL_DIM = 2048
NUM_HEADS = 16
HEAD_DIM = 128
BLOCK_LEN = 64
CONV_TAPS = 4


def setup_inputs(seed: int = 0, part: int = 0) -> dict:
    part_key = jax.random.fold_in(jax.random.key(seed), part)
    data_keys = jax.random.split(part_key, 2)
    weight_keys = jax.random.split(jax.random.key(seed + 1), 10)
    w_scale = MODEL_DIM ** -0.5
    act_shape = (BATCH_SIZE, SEQ_LEN, MODEL_DIM)
    square = (MODEL_DIM, MODEL_DIM)
    taps_shape = (CONV_TAPS, MODEL_DIM)

    def normal_bf16(rand_key, arr_shape, arr_scale):
        return (jax.random.normal(rand_key, arr_shape, jnp.float32) * arr_scale).astype(jnp.bfloat16)

    norm_draw = 0.3 + jax.random.normal(weight_keys[9], (HEAD_DIM,), jnp.float32)
    return {
        'x_in': normal_bf16(data_keys[0], act_shape, 1.0),
        'dy_out': normal_bf16(data_keys[1], act_shape, 1.0),
        'w_query': normal_bf16(weight_keys[0], square, w_scale),
        'w_key': normal_bf16(weight_keys[1], square, w_scale),
        'w_value': normal_bf16(weight_keys[2], square, w_scale),
        'w_beta': normal_bf16(weight_keys[3], (MODEL_DIM, NUM_HEADS), w_scale),
        'conv_query': normal_bf16(weight_keys[4], taps_shape, 0.5),
        'conv_key': normal_bf16(weight_keys[5], taps_shape, 0.5),
        'conv_value': normal_bf16(weight_keys[6], taps_shape, 0.5),
        'w_gate': normal_bf16(weight_keys[7], square, w_scale),
        'norm_weight': norm_draw.astype(jnp.bfloat16),
        'w_out': normal_bf16(weight_keys[8], square, w_scale),
    }


def conv_silu(proj_in, tap_weights):
    seq_len = proj_in.shape[1]
    padded = jnp.pad(proj_in.astype(jnp.float32), ((0, 0), (CONV_TAPS - 1, 0), (0, 0)))
    conv_sum = padded[:, 0:seq_len] * tap_weights[0]
    for tap_idx in range(1, CONV_TAPS):
        conv_sum = conv_sum + padded[:, tap_idx:tap_idx + seq_len] * tap_weights[tap_idx]
    return jax.nn.silu(conv_sum)


def head_l2(values):
    shaped = values.reshape(values.shape[:-1] + (-1, HEAD_DIM))
    scaled = shaped * lax.rsqrt(jnp.sum(shaped * shaped, axis=-1, keepdims=True) + 1e-6)
    return scaled.reshape(values.shape)


def delta_rule(queries, key_vecs, values, beta_tok):
    n_seqs, seq_len, model_dim = queries.shape
    n_heads = model_dim // HEAD_DIM
    n_blocks = seq_len // BLOCK_LEN

    def to_blocks(array_in):
        return array_in.astype(jnp.float32).reshape(n_seqs, n_blocks, BLOCK_LEN, n_heads, HEAD_DIM).transpose(1, 0, 3, 2, 4)

    q_blk = to_blocks(queries)
    k_blk = to_blocks(key_vecs)
    v_blk = to_blocks(values)
    b_blk = beta_tok.astype(jnp.float32).reshape(n_seqs, n_blocks, BLOCK_LEN, n_heads).transpose(1, 0, 3, 2)
    positions = jnp.arange(BLOCK_LEN)
    strict = (positions[:, None] > positions[None, :]).astype(jnp.float32)
    inclusive = (positions[:, None] >= positions[None, :]).astype(jnp.float32)
    gram_mat = jnp.einsum('nbhca,nbhsa->nbhcs', k_blk, k_blk)
    system = jnp.eye(BLOCK_LEN, dtype=jnp.float32) + b_blk[..., None] * gram_mat * strict
    rhs_mat = jnp.concatenate([k_blk, v_blk], axis=-1) * b_blk[..., None]
    solved = jnp.linalg.solve(system, rhs_mat)
    scores = jnp.einsum('nbhca,nbhsa->nbhcs', q_blk, k_blk) * inclusive

    def scan_step(state_mat, block_in):
        w_n, u_n, q_n, k_n, s_n = block_in
        delta_mat = u_n - jnp.einsum('bhca,bhae->bhce', w_n, state_mat)
        out_n = jnp.einsum('bhca,bhae->bhce', q_n, state_mat) + jnp.einsum('bhcs,bhse->bhce', s_n, delta_mat)
        state_mat = state_mat + jnp.einsum('bhca,bhce->bhae', k_n, delta_mat)
        return state_mat, out_n

    init_state = jnp.zeros((n_seqs, n_heads, HEAD_DIM, HEAD_DIM), jnp.float32)
    block_outs = lax.scan(scan_step, init_state, (solved[..., :HEAD_DIM], solved[..., HEAD_DIM:], q_blk, k_blk, scores))[1]
    return block_outs.transpose(1, 0, 3, 2, 4).reshape(n_seqs, seq_len, model_dim)


def layer_forward(x_f, weights):
    w_query, w_key, w_value, w_beta, conv_query, conv_key, conv_value, w_gate, norm_weight, w_out = weights
    n_seqs, seq_len, model_dim = x_f.shape
    flat_x = x_f.reshape(n_seqs * seq_len, model_dim)

    def project(weight):
        return jnp.dot(flat_x, weight, preferred_element_type=jnp.float32).astype(jnp.bfloat16).reshape(n_seqs, seq_len, -1)

    queries = head_l2(conv_silu(project(w_query), conv_query)).astype(jnp.bfloat16)
    key_vecs = head_l2(conv_silu(project(w_key), conv_key)).astype(jnp.bfloat16)
    values = conv_silu(project(w_value), conv_value).astype(jnp.bfloat16)
    beta_tok = jax.nn.sigmoid(project(w_beta).astype(jnp.float32)).astype(jnp.bfloat16)
    attn_out = delta_rule(queries, key_vecs, values, beta_tok).astype(jnp.bfloat16)
    gate_pre = project(w_gate)
    shaped = attn_out.astype(jnp.float32).reshape(n_seqs, seq_len, -1, HEAD_DIM)
    normed = shaped * lax.rsqrt(jnp.mean(shaped * shaped, axis=-1, keepdims=True) + 1e-5) * norm_weight
    hidden = (normed.reshape(n_seqs, seq_len, model_dim) * jax.nn.silu(gate_pre.astype(jnp.float32))).astype(jnp.bfloat16)
    y_flat = jnp.dot(hidden.reshape(n_seqs * seq_len, model_dim), w_out, preferred_element_type=jnp.float32)
    return y_flat.astype(jnp.bfloat16).reshape(n_seqs, seq_len, model_dim)


def reference(x_in, dy_out, w_query, w_key, w_value, w_beta, conv_query, conv_key, conv_value, w_gate, norm_weight, w_out):
    weights = tuple(array_in.astype(jnp.float32) for array_in in (w_query, w_key, w_value, w_beta, conv_query, conv_key, conv_value, w_gate, norm_weight, w_out))
    y_out, pullback = jax.vjp(layer_forward, x_in.astype(jnp.float32), weights)
    dx_f, grad_list = pullback(dy_out)
    return (y_out, dx_f.astype(jnp.bfloat16), grad_list[0], grad_list[1], grad_list[2], grad_list[3], grad_list[4], grad_list[5], grad_list[6], grad_list[7], grad_list[8], grad_list[9])
```

```python
import functools
import itertools
import jax
import jax.numpy as jnp
from jax import lax
from jax.experimental import pallas as pl
from jax.experimental.pallas import tpu as pltpu
from jax.sharding import PartitionSpec as P

HEAD_DIM = 128
BLOCK_LEN = 64
CHUNK = 128
CONV_TAPS = 4
F32 = jnp.float32
BF16 = jnp.bfloat16


def mm(lhs, rhs):
    return lax.dot_general(lhs, rhs, (((1,), (0,)), ((), ())), preferred_element_type=F32)


def mm_nt(lhs, rhs):
    return lax.dot_general(lhs, rhs, (((1,), (1,)), ((), ())), preferred_element_type=F32)


def mm_tn(lhs, rhs):
    return lax.dot_general(lhs, rhs, (((0,), (0,)), ((), ())), preferred_element_type=F32)


def split(value):
    high = value.astype(BF16)
    return high, (value - high.astype(F32)).astype(BF16)


def cat0(*parts):
    return jnp.concatenate(parts, axis=0)


def cat1(*parts):
    return jnp.concatenate(parts, axis=1)


def sigmoid(value):
    return 0.5 + 0.5 * jnp.tanh(0.5 * value)


def lane_sum(value):
    return jnp.sum(value, axis=-1, keepdims=True)


def row_sum8(value):
    return jnp.sum(value.reshape(value.shape[0] // 8, 8, value.shape[1]), axis=0)


def iota2(rows, cols, axis):
    return lax.broadcasted_iota(jnp.int32, (rows, cols), axis)


def interleave(main, side=(), pace=0):
    def advance(gen):
        for _ in gen:
            return True
        return False

    stages = itertools.chain.from_iterable(side)
    main = list(main)
    while main:
        main = [gen for gen in main if advance(gen)]
        for _ in range(pace):
            advance(stages)


def cols_of(head):
    return slice(head * HEAD_DIM, (head + 1) * HEAD_DIM)


def tokens_at(ref, cols):
    part = ref[:, 0, :, cols]
    return part.reshape(part.shape[0] * part.shape[1], part.shape[2])


def put_tokens(ref, cols, value):
    ref[:, 0, :, cols] = value.reshape(ref.shape[0], ref.shape[2], HEAD_DIM).astype(ref.dtype)


PACE = 6


def pair_rows(index, n_all):
    return pl.ds(index, BLOCK_LEN, stride=n_all)


def conv_views(scratch, slot, proj):
    n_tok = proj.shape[0]
    scratch[slot, 8:8 + n_tok] = proj
    return [scratch[slot, 8 - back:8 - back + n_tok] for back in range(CONV_TAPS - 1, 0, -1)] + [proj]


def conv_half(views, half_taps):
    total = views[0] * half_taps[0:1]
    for tap in range(1, CONV_TAPS):
        total = total + views[tap] * half_taps[tap:tap + 1]
    return total


def prep_kernel(n_heads, pq_ref, pk_ref, pv_ref, logit_ref, taps_ref, q_ref, k_ref, v_ref, l_ref, ck_ref, cq_ref, cv_ref, shift_ref):
    n_pairs = l_ref.shape[1] // (BLOCK_LEN * n_heads)
    strict = iota2(BLOCK_LEN, 2 * BLOCK_LEN, 0) > (iota2(BLOCK_LEN, 2 * BLOCK_LEN, 1) & (BLOCK_LEN - 1))
    left = iota2(BLOCK_LEN, 2 * BLOCK_LEN, 1) < BLOCK_LEN

    @pl.when(pl.program_id(0) == 0)
    def _():
        shift_ref[:, 0:8] = jnp.zeros((shift_ref.shape[0], 8, HEAD_DIM), F32)

    beta_all = sigmoid(tokens_at(logit_ref, slice(0, HEAD_DIM)).astype(F32)).astype(BF16).astype(F32)

    def one_head(head):
        cols = cols_of(head)
        for branch, (p_ref, out_ref, c_ref) in enumerate(((pk_ref, k_ref, ck_ref), (pq_ref, q_ref, cq_ref), (pv_ref, v_ref, cv_ref))):
            views = conv_views(shift_ref, 3 * head + branch, tokens_at(p_ref, cols).astype(F32))
            half_conv = conv_half(views, taps_ref[branch, :, cols])
            put_tokens(c_ref, cols, half_conv)
            act = half_conv + half_conv * jnp.tanh(half_conv)
            if branch < 2:
                act = act * lax.rsqrt(lane_sum(act * act) + 1e-6)
            act = act.astype(BF16)
            put_tokens(out_ref, cols, act)
            if branch == 0:
                keys = act
            yield
        for pair in range(n_pairs):
            two = keys[pair * CHUNK:(pair + 1) * CHUNK]
            gram = mm_nt(two, two)
            betas = beta_all[pair * CHUNK:(pair + 1) * CHUNK, head:head + 1]
            low = jnp.where(left, gram[:BLOCK_LEN] * betas[:BLOCK_LEN], gram[BLOCK_LEN:] * betas[BLOCK_LEN:])
            l_ref[0, pair_rows(head * n_pairs + pair, n_heads * n_pairs), :] = jnp.where(strict, low, 0.0)
            yield

    interleave(map(one_head, range(n_heads)))


def invert_kernel(per_seq, l_ref, t_ref, low_ref, inv_ref):
    group = 8
    n_groups = BLOCK_LEN // group
    n_seqs, lanes = l_ref.shape[0], l_ref.shape[0] * per_seq
    sub = iota2(group, lanes, 0)
    eye = (iota2(lanes, lanes, 0) == iota2(lanes, lanes, 1)).astype(BF16)
    eyes = cat1(eye, eye)

    def load_row(row):
        slab = l_ref[:, row * per_seq:(row + 1) * per_seq, :].reshape(lanes, CHUNK)
        low_ref[row] = mm_nt_eye(slab)

    def mm_nt_eye(slab):
        high, low = split(slab)
        return mm_nt(eyes, cat1(high, low))

    def store_row(row):
        t_ref[:, row * per_seq:(row + 1) * per_seq, :] = inv_ref[row].T.reshape(n_seqs, per_seq, CHUNK)

    for rb in range(n_groups):
        for r in range(group):
            load_row(rb * group + r)
        for side in range(2):
            base = side * BLOCK_LEN
            rows = [[None] * (rb + 1) for _ in range(group)]
            for r in range(group):
                row = rb * group + r
                for jg in range(rb):
                    total = None
                    for m in range(jg * group, rb * group):
                        term = low_ref[row, base + m:base + m + 1, :] * inv_ref[m, base + jg * group:base + (jg + 1) * group, :]
                        total = term if total is None else total + term
                    rows[r][jg] = -total
                rows[r][rb] = jnp.where(sub == r, 1.0, 0.0).astype(F32)
            for r in range(group):
                row = rb * group + r
                for m in range(r):
                    factor = low_ref[row, base + rb * group + m:base + rb * group + m + 1, :]
                    for jg in range(rb + 1):
                        rows[r][jg] = rows[r][jg] - factor * rows[m][jg]
                for jg in range(n_groups):
                    value = rows[r][jg] if jg <= rb else jnp.zeros((group, lanes), F32)
                    inv_ref[row, base + jg * group:base + (jg + 1) * group, :] = value
        for r in range(group):
            store_row(rb * group + r)


def tri_masks():
    rows, cols = iota2(CHUNK, CHUNK, 0), iota2(CHUNK, CHUNK, 1)
    return rows >= cols, rows > cols


def merge_inverse(t_pair, gram, betas):
    left = iota2(BLOCK_LEN, CHUNK, 1) < BLOCK_LEN
    zero = jnp.zeros((BLOCK_LEN, CHUNK), BF16)
    bottom = jnp.where(left, 0.0, t_pair)
    cross_h, cross_l = split(jnp.where(left, gram[BLOCK_LEN:] * betas[BLOCK_LEN:], 0.0))
    top_h, top_l = split(jnp.where(left, t_pair, 0.0))
    bottom_h, bottom_l = split(bottom)
    inner = mm(cat1(cross_h, cross_l), cat0(top_h, zero, top_h, zero)) + mm(cross_h, cat0(top_l, zero))
    yield
    inner_h, inner_l = split(inner)
    outer = mm(cat1(bottom_h, bottom_l), cat0(zero, inner_h, zero, inner_h)) + mm(bottom_h, cat0(zero, inner_l))
    yield
    bot_h, bot_l = split(bottom - outer)
    return cat0(top_h, bot_h), cat0(top_l, bot_l)


def forward_kernel(n_heads, mate_ref, q_ref, k_ref, v_ref, z_ref, logit_ref, norm_ref, t_ref, h_ref, send_ref, o_ref, u_ref, s_ref, inv_ref):
    n_chunks = u_ref.shape[2]
    incl, _ = tri_masks()
    norm = norm_ref[...]
    beta_all = sigmoid(tokens_at(logit_ref, slice(0, HEAD_DIM)).astype(F32)).astype(BF16).astype(F32)

    def one_head(head):
        cols = cols_of(head)
        queries, keys, values = tokens_at(q_ref, cols), tokens_at(k_ref, cols), tokens_at(v_ref, cols)
        outs, scores, inverses, betas = [], [], [], []
        for c in range(n_chunks):
            rows = slice(c * CHUNK, (c + 1) * CHUNK)
            k_c = keys[rows]
            both = mm_nt(cat0(queries[rows], k_c), k_c)
            b_c = beta_all[rows, head:head + 1]
            betas.append(b_c)
            yield
            scores.append(jnp.where(incl, both[:CHUNK], 0.0).astype(BF16))
            inv_h, inv_l = yield from merge_inverse(t_ref[0, pair_rows(head * n_chunks + c, n_heads * n_chunks), :], both[CHUNK:], b_c)
            inv_ref[0, head, c, :, :CHUNK] = inv_h
            inv_ref[0, head, c, :, CHUNK:] = inv_l
            inverses.append((inv_h, inv_l))
        state_h = state_l = None
        for c in range(n_chunks):
            rows = slice(c * CHUNK, (c + 1) * CHUNK)
            q_c, k_c = queries[rows], keys[rows]
            inv_h, inv_l = inverses[c]
            rhs = values[rows].astype(F32)
            if c > 0:
                through = mm(cat1(cat0(q_c, k_c), cat0(q_c, k_c)), cat0(state_h, state_l))
                yield
                rhs = rhs - through[CHUNK:]
            rhs_h, rhs_l = split(rhs * betas[c])
            solved = mm(cat1(inv_h, inv_l), cat0(rhs_h, rhs_h)) + mm(inv_h, rhs_l)
            yield
            u_h, u_l = split(solved)
            u_ref[0, head, c, :, :CHUNK] = u_h
            u_ref[0, head, c, :, CHUNK:] = u_l
            if c + 1 < n_chunks:
                update = mm_tn(cat0(k_c, k_c), cat0(u_h, u_l))
                yield
                state = update if c == 0 else state + update
                state_h, state_l = split(state)
                s_ref[0, head, c, :, :CHUNK] = state_h
                s_ref[0, head, c, :, CHUNK:] = state_l
            out = mm(cat1(scores[c], scores[c]), cat0(u_h, u_l))
            if c > 0:
                out = out + through[:CHUNK]
            outs.append(out)
        yield
        out = cat0(*outs).astype(BF16)
        put_tokens(o_ref, cols, out)
        out = out.astype(F32)
        normed = out * lax.rsqrt(lane_sum(out * out) * (1.0 / HEAD_DIM) + 1e-5) * norm
        yield
        half_gate = 0.5 * tokens_at(z_ref, cols).astype(F32)
        put_tokens(h_ref, cols, normed * (half_gate + half_gate * jnp.tanh(half_gate)))

    interleave(map(one_head, range(n_heads)))
    send_ref[0] = h_ref[mate_ref[0], 0]


def backward_kernel(n_heads, mate_ref, dh_ref, o_ref, pq_ref, pk_ref, pv_ref, z_ref, logit_ref, q_ref, k_ref, v_ref, ck_ref, cq_ref, cv_ref, norm_ref, taps_ref,
                    u_ref, s_ref, inv_ref, dp_ref, send_ref, dnorm_ref, dtaps_ref, after_ref, held_ref):
    n_chunks = u_ref.shape[2]
    incl, strict = tri_masks()
    norm = norm_ref[...]
    n_tok = n_chunks * CHUNK
    width = n_heads * HEAD_DIM
    head_lane = iota2(n_tok, HEAD_DIM, 1)

    @pl.when(pl.program_id(0) == 0)
    def _():
        dnorm_ref[...] = jnp.zeros_like(dnorm_ref)
        dtaps_ref[...] = jnp.zeros_like(dtaps_ref)
        after_ref[:, n_tok:n_tok + 8] = jnp.zeros((after_ref.shape[0], 8, HEAD_DIM), F32)
        held_ref[...] = jnp.zeros_like(held_ref)

    for at in range(3 * width, held_ref.shape[1], HEAD_DIM):
        put_tokens(dp_ref, slice(at, at + HEAD_DIM), held_ref[:, at:at + HEAD_DIM])

    sig_beta = sigmoid(tokens_at(logit_ref, slice(0, HEAD_DIM)).astype(F32))
    beta_all = sig_beta.astype(BF16).astype(F32)
    d_beta_cols = [None] * n_heads
    d_norms = [None] * n_heads

    def one_head(head):
        cols = cols_of(head)
        d_hid = tokens_at(dh_ref, cols).astype(F32)
        out = tokens_at(o_ref, cols).astype(F32)
        half_gate = 0.5 * tokens_at(z_ref, cols).astype(F32)
        inv_rms = lax.rsqrt(lane_sum(out * out) * (1.0 / HEAD_DIM) + 1e-5)
        yield
        tanh = jnp.tanh(half_gate)
        up = 1.0 + tanh
        act = half_gate * up
        slope = up + act * (1.0 - tanh)
        unit = out * inv_rms
        d_scaled = d_hid * act
        d_norms[head] = row_sum8(d_scaled * unit)
        d_gate = (d_hid * (unit * (0.5 * norm)) * slope).astype(BF16)
        d_unit = d_scaled * norm
        inner = lane_sum(d_unit * unit) * (1.0 / HEAD_DIM)
        yield
        d_out = ((d_unit - unit * inner) * inv_rms).astype(BF16)

        queries, keys, values = tokens_at(q_ref, cols), tokens_at(k_ref, cols), tokens_at(v_ref, cols)
        d_state = None
        d_qs, d_ks, d_vs, d_betas = [], [], [], []
        for c in reversed(range(n_chunks)):
            rows = slice(c * CHUNK, (c + 1) * CHUNK)
            q_c, k_c, do_c = queries[rows], keys[rows], d_out[rows]
            b_c = beta_all[rows, head:head + 1]
            u_cat = u_ref[0, head, c]
            u_h = u_cat[:, :CHUNK]
            inv = inv_ref[0, head, c]
            inv_h, inv_l = inv[:, :CHUNK], inv[:, CHUNK:]
            both = mm_nt(cat0(q_c, k_c), k_c)
            yield
            scores = jnp.where(incl, both[:CHUNK], 0.0).astype(BF16)
            gram = both[CHUNK:]
            d_u = mm_tn(scores, do_c)
            if d_state is not None:
                ds_h, ds_l = split(d_state)
                d_u = d_u + mm(cat1(k_c, k_c), cat0(ds_h, ds_l))
            yield
            du_h, du_l = split(d_u)
            d_rhs = mm_tn(cat0(inv_h, inv_l), cat0(du_h, du_h)) + mm_tn(inv_h, du_l)
            rhs = values[rows].astype(F32)
            if c > 0:
                state = s_ref[0, head, c - 1]
                rhs = rhs - mm(cat1(k_c, k_c), cat0(state[:, :CHUNK], state[:, CHUNK:]))
            yield
            d_val = d_rhs * b_c
            d_vs.append(d_val)
            left = cat0(do_c, d_rhs.astype(BF16))
            pair = mm_nt(cat1(left, left), u_cat)
            if c > 0:
                left = cat0(do_c, -d_val.astype(BF16))
                more = mm_nt(cat1(left, left), state)
                step = mm_tn(cat0(q_c, k_c), left)
            yield
            d_scores = jnp.where(incl, pair[:CHUNK], 0.0).astype(BF16)
            d_low = jnp.where(strict, -pair[CHUNK:], 0.0)
            d_betas.append(lane_sum(d_low * gram + d_rhs * rhs))
            d_gram = (d_low * b_c).astype(BF16)
            mixed = cat0(d_scores, d_gram)
            first = mm(mixed, k_c)
            d_q = first[:CHUNK]
            d_k = first[CHUNK:] + mm_tn(mixed, cat0(q_c, k_c))
            if c > 0:
                d_q = d_q + more[:CHUNK]
                d_k = d_k + more[CHUNK:]
            if d_state is not None:
                d_k = d_k + mm_nt(cat1(u_h, u_h), cat1(ds_h, ds_l))
            if c > 0:
                d_state = step if d_state is None else d_state + step
            d_qs.append(d_q)
            d_ks.append(d_k)
            yield
        d_beta_cols[head] = cat0(*d_betas[::-1])
        for branch, parts in enumerate((d_qs, d_ks, d_vs)):
            held_ref[:, part_cols(branch, head)] = cat0(*parts[::-1]).astype(BF16)
        held_ref[:, part_cols(3, head)] = d_gate

    def part_cols(branch, head):
        return slice(branch * width + head * HEAD_DIM, branch * width + (head + 1) * HEAD_DIM)

    def conv_branch(head, branch):
        p_ref, c_ref, place = ((pk_ref, ck_ref, 1), (pq_ref, cq_ref, 0), (pv_ref, cv_ref, 2))[branch]
        slot, cols = 3 * head + branch, cols_of(head)
        half_taps = taps_ref[branch, :, cols]
        half_conv = tokens_at(c_ref, cols)
        tanh = jnp.tanh(half_conv)
        up = 1.0 + tanh
        act = half_conv * up
        slope = up + act * (1.0 - tanh)
        d_act = held_ref[:, part_cols(place, head)].astype(F32)
        if branch < 2:
            inv_len = lax.rsqrt(lane_sum(act * act) + 1e-6)
            unit = act * inv_len
            d_act = (d_act - unit * lane_sum(d_act * unit)) * inv_len
        d_conv = d_act * slope
        yield
        after_ref[slot, 0:n_tok] = d_conv
        proj = tokens_at(p_ref, cols).astype(F32)
        d_proj = None
        for tap in reversed(range(CONV_TAPS)):
            ahead = CONV_TAPS - 1 - tap
            later = after_ref[slot, ahead:ahead + n_tok] if ahead else d_conv
            term = later * half_taps[tap:tap + 1]
            d_proj = term if d_proj is None else d_proj + term
            dtaps_ref[branch, tap, :, cols] += row_sum8(proj * later)
        put_tokens(dp_ref, part_cols(place, head), d_proj)
        yield

    units = [conv_branch(head, branch) for head in range(n_heads) for branch in range(3)]
    interleave(map(one_head, range(n_heads)), units, PACE)
    d_beta = jnp.zeros((n_tok, HEAD_DIM), F32)
    for head in range(n_heads):
        d_beta = jnp.where(head_lane == head, d_beta_cols[head], d_beta)
    held_ref[:, 4 * width:] = (d_beta.astype(BF16).astype(F32) * sig_beta * (1.0 - sig_beta)).astype(BF16)
    total = d_norms[0]
    for part in d_norms[1:]:
        total = total + part
    dnorm_ref[...] += jnp.where(pl.program_id(0) < pl.num_programs(0) - 1, total, 0.0)
    send_ref[0] = dp_ref[mate_ref[0], 0]


def params(semantics=('arbitrary',)):
    return pltpu.CompilerParams(dimension_semantics=semantics, vmem_limit_bytes=60 * 1024 * 1024)


def seq_spec(n_blocks, width, col=0, first=0, seq_of=lambda n: n):
    return pl.BlockSpec((n_blocks, 1, BLOCK_LEN, width), lambda n, *_: (0, seq_of(n + first), 0, col))


def lead_spec(shape, first=0, seq_of=lambda n: n):
    return pl.BlockSpec(shape, lambda n, *_: (seq_of(n + first),) + (0,) * (len(shape) - 1))


def fixed(shape):
    return pl.BlockSpec(shape, lambda *_: (0,) * len(shape))


def full_once(shape):
    return pl.BlockSpec(shape, lambda *_: (0,) * len(shape), pipeline_mode=pl.Buffered(1))


ANY = pl.BlockSpec(memory_space=pl.ANY)
TWO_LOOPS = ('arbitrary', 'arbitrary')


def head_spec(n_heads, n_chunks, rows, width, **more):
    return lead_spec((1, n_heads, n_chunks, rows, width), **more)


def cost(flops, nbytes):
    return pl.CostEstimate(flops=int(flops), bytes_accessed=int(nbytes), transcendentals=0)


def shift_scratch(n_heads, n_blocks):
    return pltpu.VMEM((3 * n_heads, n_blocks * BLOCK_LEN + 8, HEAD_DIM), F32)


def prep(proj, half_taps, width, first=0, count=None, begun=()):
    n_blocks, n_seqs = proj.shape[:2]
    count = n_seqs if count is None else count
    n_heads = width // HEAD_DIM
    n_pairs = n_blocks // 2
    act, conv = (jax.ShapeDtypeStruct((n_blocks, n_seqs, BLOCK_LEN, width), dtype) for dtype in (BF16, F32))
    sspec = functools.partial(seq_spec, n_blocks, width, first=first)

    def kernel(pq_ref, pk_ref, pv_ref, logit_ref, taps_ref, *refs):
        prep_kernel(n_heads, pq_ref, pk_ref, pv_ref, logit_ref, taps_ref, *refs[len(begun):])

    return pl.pallas_call(
        kernel, grid=(count,), name='prep',
        in_specs=[sspec(0), sspec(1), sspec(2), seq_spec(n_blocks, HEAD_DIM, 4 * n_heads, first), fixed(half_taps.shape)]
        + [ANY] * len(begun),
        out_specs=[sspec(0), sspec(0), sspec(0), lead_spec((1, BLOCK_LEN * n_heads * n_pairs, CHUNK), first)] + [sspec(0)] * 3,
        out_shape=[act, act, act, jax.ShapeDtypeStruct((n_seqs, BLOCK_LEN * n_heads * n_pairs, CHUNK), F32)] + [conv] * 3,
        scratch_shapes=[shift_scratch(n_heads, n_blocks)],
        input_output_aliases={5 + index: index for index in range(len(begun))},
        cost_estimate=cost(60e6 * count * n_heads, 8e5 * count * n_heads), compiler_params=params(),
    )(proj, proj, proj, proj, half_taps, *begun)


def invert(low):
    n_seqs, n_rows, _ = low.shape
    per_seq = n_rows // BLOCK_LEN
    group = CHUNK // per_seq
    spec = lead_spec((group, n_rows, CHUNK))
    return pl.pallas_call(
        functools.partial(invert_kernel, per_seq), grid=(n_seqs // group,), name='invert', in_specs=[spec], out_specs=spec,
        out_shape=jax.ShapeDtypeStruct(low.shape, F32), scratch_shapes=[pltpu.VMEM((BLOCK_LEN, CHUNK, CHUNK), F32)] * 2,
        cost_estimate=cost(28e6 * n_seqs * per_seq, 8 * low.size), compiler_params=params(),
    )(low)


def delta_forward(mate, queries, keys, values, proj, norm, inverse):
    n_blocks, n_seqs, _, width = queries.shape
    n_heads = width // HEAD_DIM
    n_chunks = n_blocks * BLOCK_LEN // CHUNK
    act, send = (jax.ShapeDtypeStruct(queries.shape[cut:], BF16) for cut in range(2))
    sspec = functools.partial(seq_spec, n_blocks, width)
    saved, states = (jax.ShapeDtypeStruct((n_seqs, n_heads, count, CHUNK, 2 * CHUNK), BF16) for count in (n_chunks, n_chunks - 1))
    wide, narrow = (head_spec(n_heads, count, CHUNK, 2 * CHUNK) for count in (n_chunks, n_chunks - 1))
    grid_spec = pltpu.PrefetchScalarGridSpec(
        num_scalar_prefetch=1, grid=(n_seqs,),
        in_specs=[sspec(0)] * 3 + [sspec(3), seq_spec(n_blocks, HEAD_DIM, 4 * n_heads), fixed((1, HEAD_DIM)), lead_spec((1,) + inverse.shape[1:])],
        out_specs=[sspec(0), lead_spec((1, BLOCK_LEN, width)), sspec(0), wide, narrow, wide])
    return pl.pallas_call(
        functools.partial(forward_kernel, n_heads), grid_spec=grid_spec, name='delta_fwd', out_shape=[act, send, act, saved, states, saved],
        cost_estimate=cost(150e6 * n_seqs * n_heads, 8e5 * n_seqs * n_heads), compiler_params=params(),
    )(mate, queries, keys, values, proj, proj, norm, inverse)


def layer_backward(mate, d_hid, out, proj, acts, convs, norm, half_taps, solved, states, inverse):
    n_blocks, n_seqs, _, width = d_hid.shape
    n_heads = width // HEAD_DIM
    n_chunks = n_blocks * BLOCK_LEN // CHUNK
    wide_width = proj.shape[-1]
    now = {'seq_of': lambda n: jnp.minimum(n, n_seqs - 1)}
    before = {'seq_of': lambda n: jnp.maximum(n - 1, 0)}
    now_spec = functools.partial(seq_spec, n_blocks, width, **now)
    before_spec = functools.partial(seq_spec, n_blocks, width, **before)
    wide, narrow = (head_spec(n_heads, count, CHUNK, 2 * CHUNK, **now) for count in (n_chunks, n_chunks - 1))
    norm_shape, taps_shape = (8, HEAD_DIM), (3, CONV_TAPS, 8, width)
    grid_spec = pltpu.PrefetchScalarGridSpec(
        num_scalar_prefetch=1, grid=(n_seqs + 1,),
        in_specs=[now_spec()] * 2 + [before_spec(col) for col in range(3)] + [now_spec(3), seq_spec(n_blocks, HEAD_DIM, 4 * n_heads, **now)] + [now_spec()] * 3
        + [before_spec()] * 3 + [fixed(norm.shape), fixed(half_taps.shape), wide, narrow, wide],
        out_specs=[seq_spec(n_blocks, wide_width, **before), lead_spec((1, BLOCK_LEN, wide_width), **before), fixed(norm_shape), fixed(taps_shape)],
        scratch_shapes=[shift_scratch(n_heads, n_blocks), pltpu.VMEM((n_blocks * BLOCK_LEN, wide_width), BF16)])
    return pl.pallas_call(
        functools.partial(backward_kernel, n_heads), grid_spec=grid_spec, name='layer_bwd',
        out_shape=[jax.ShapeDtypeStruct(proj.shape, BF16), jax.ShapeDtypeStruct(proj.shape[1:], BF16), jax.ShapeDtypeStruct(norm_shape, F32),
                   jax.ShapeDtypeStruct(taps_shape, F32)],
        cost_estimate=cost(350e6 * n_seqs * n_heads, 12e5 * n_seqs * n_heads), compiler_params=params(),
    )(mate, d_hid, out, *[proj] * 5, *acts, *convs, norm, half_taps, solved, states, inverse)


PIECE = 1024


def pieces(size, body):
    def step(index, carry):
        body(pl.multiple_of(index * PIECE, PIECE))
        return carry

    lax.fori_loop(0, size // PIECE, step, 0)


def once(shape, index_map):
    return pl.BlockSpec(shape, index_map, pipeline_mode=pl.Buffered(1))


def flat(value):
    return value.reshape(value.shape[0] * value.shape[1], value.shape[2])


def project(where, x_part, weights, w_beta, first=0, begun=None, n_blocks=4, n_seqs=32):
    count, _, model_dim = x_part.shape
    half = model_dim // 2
    tile = 8
    width = 4 * half + HEAD_DIM

    def kernel(where_ref, x_ref, wb_ref, *refs):
        p_ref, held, sems = refs[-3:]
        mine = pl.multiple_of(where_ref[1] * half, half)
        loads = [pltpu.make_async_copy(w_ref.at[:, pl.ds(mine, half)], held.at[branch], sems.at[branch]) for branch, w_ref in enumerate(refs[:4])]
        begins = pl.program_id(0) == 0

        @pl.when(begins)
        def _():
            loads[0].start()

        p_ref[0, :, :, 4 * half:] = mm(flat(x_ref[...]), wb_ref[...]).astype(BF16).reshape(tile, BLOCK_LEN, HEAD_DIM)

        def one_branch(branch, carry):
            for index, load in enumerate(loads):
                @pl.when(jnp.logical_and(begins, branch == index))
                def _(index=index, load=load):
                    load.wait()
                    if index + 1 < len(loads):
                        loads[index + 1].start()

            res = mm(flat(x_ref[...]), held[branch]).astype(BF16)
            p_ref[0, :, :, pl.ds(pl.multiple_of(branch * half, half), half)] = res.reshape(tile, BLOCK_LEN, half)
            return carry

        lax.fori_loop(0, 4, one_branch, 0)

    extra = [] if begun is None else [begun]
    grid_spec = pltpu.PrefetchScalarGridSpec(
        num_scalar_prefetch=1, grid=(count // tile,),
        in_specs=[lead_spec((tile, BLOCK_LEN, model_dim)), full_once(w_beta.shape)] + [ANY] * (4 + len(extra)),
        out_specs=pl.BlockSpec((1, tile, BLOCK_LEN, width), lambda t, where: (where[0], t + first // tile, 0, 0)),
        scratch_shapes=[pltpu.VMEM((4, model_dim, half), BF16), pltpu.SemaphoreType.DMA((4,))])
    return pl.pallas_call(
        kernel, grid_spec=grid_spec, name='project', out_shape=jax.ShapeDtypeStruct((n_blocks, n_seqs, BLOCK_LEN, width), BF16),
        input_output_aliases={7: 0} if extra else {},
        cost_estimate=cost(2 * count * BLOCK_LEN * model_dim * width, x_part.size * 4), compiler_params=params(),
    )(where, x_part, w_beta, *weights, *extra)


def hidden_grad(core, dy_all, w_out):
    n_blocks, n_seqs, _, model_dim = dy_all.shape
    half = model_dim // 2
    tile = 16

    def kernel(core_ref, dy_ref, w_ref, dh_ref):
        def piece(at):
            res = mm_nt(flat(dy_ref[0]), w_ref[pl.ds(at, PIECE), :]).astype(BF16)
            dh_ref[0, :, :, pl.ds(at, PIECE)] = res.reshape(tile, BLOCK_LEN, PIECE)

        pieces(half, piece)

    grid_spec = pltpu.PrefetchScalarGridSpec(
        num_scalar_prefetch=1, grid=(n_blocks, n_seqs // tile),
        in_specs=[pl.BlockSpec((1, tile, BLOCK_LEN, model_dim), lambda b, t, core: (b, t, 0, 0)), once((half, model_dim), lambda b, t, core: (core[0], 0))],
        out_specs=pl.BlockSpec((1, tile, BLOCK_LEN, half), lambda b, t, core: (b, t, 0, 0)))
    return pl.pallas_call(
        kernel, grid_spec=grid_spec, name='hidden_grad', out_shape=jax.ShapeDtypeStruct((n_blocks, n_seqs, BLOCK_LEN, half), BF16),
        cost_estimate=cost(dy_all.size * model_dim, dy_all.size * 4), compiler_params=params(TWO_LOOPS),
    )(core, dy_all, w_out)


def output_dot(place, hidden, hid_mate, w_out):
    _, n_seqs, _, half = hidden.shape
    model_dim = 2 * half
    tile = 16

    def kernel(place_ref, own_ref, mate_ref, w_ref, y_ref):
        mine = pl.multiple_of(place_ref[1] * half, half)
        other = pl.multiple_of(half - place_ref[1] * half, half)

        def piece(at):
            res = mm(flat(own_ref[0]), w_ref[pl.ds(mine, half), pl.ds(at, PIECE)]) + mm(flat(mate_ref[...]), w_ref[pl.ds(other, half), pl.ds(at, PIECE)])
            y_ref[:, :, pl.ds(at, PIECE)] = res.astype(BF16).reshape(tile, BLOCK_LEN, PIECE)

        pieces(model_dim, piece)

    grid_spec = pltpu.PrefetchScalarGridSpec(
        num_scalar_prefetch=1, grid=(n_seqs // tile,),
        in_specs=[pl.BlockSpec((1, tile, BLOCK_LEN, half), lambda t, place: (place[0], t, 0, 0)),
                  lead_spec((tile, BLOCK_LEN, half)), full_once((model_dim, model_dim))],
        out_specs=lead_spec((tile, BLOCK_LEN, model_dim)))
    return pl.pallas_call(
        kernel, grid_spec=grid_spec, name='output_dot', out_shape=jax.ShapeDtypeStruct((n_seqs, BLOCK_LEN, model_dim), BF16),
        cost_estimate=cost(2 * n_seqs * BLOCK_LEN * model_dim * model_dim, 4 * n_seqs * BLOCK_LEN * model_dim), compiler_params=params(),
    )(place, hidden, hid_mate, w_out)


def input_grad(place, d_proj, dp_mate, weights, wb_mine, wb_mate, grad_mates, out_mate, wholes, out_whole):
    _, n_seqs, _, width = d_proj.shape
    model_dim = weights[0].shape[0]
    half = model_dim // 2
    tile, rows = 16, 512
    n_rows = model_dim // rows
    steps = n_rows * (n_seqs // tile)
    lines, out_lines = model_dim // steps, half // steps

    def kernel(place_ref, own_ref, mate_ref, *refs):
        w_refs, (wbo_ref, wbm_ref), sources = refs[:4], refs[4:6], refs[6:11]
        dx_ref, *targets = refs[-6:]
        mine = pl.multiple_of(place_ref[1] * half, half)
        other = pl.multiple_of(half - place_ref[1] * half, half)

        def part(cols, w_own, w_mate):
            return mm_nt(flat(own_ref[0, :, :, cols]), w_own) + mm_nt(flat(mate_ref[:, :, cols]), w_mate)

        res = part(slice(4 * half, width), wbo_ref[...], wbm_ref[...])
        for branch, w_ref in enumerate(w_refs):
            res = res + part(slice(branch * half, (branch + 1) * half), w_ref[:, pl.ds(mine, half)], w_ref[:, pl.ds(other, half)])
        dx_ref[...] = res.astype(BF16).reshape(tile, BLOCK_LEN, rows)
        for source, target in zip(sources, targets):
            target[...] = source[...]

    def by_step(shape, col_of, row_shift=lambda place: 0):
        return pl.BlockSpec(shape, lambda t, d, place: (t * n_rows + d + row_shift(place), col_of(place)))

    def by_rows(cols):
        return pl.BlockSpec((rows, cols), lambda t, d, place: (d, 0))

    grid_spec = pltpu.PrefetchScalarGridSpec(
        num_scalar_prefetch=1, grid=(n_seqs // tile, n_rows),
        in_specs=[once((1, tile, BLOCK_LEN, width), lambda t, d, place: (place[0], t, 0, 0)), once((tile, BLOCK_LEN, width), lambda t, d, place: (t, 0, 0))]
        + [by_rows(model_dim)] * 4 + [by_rows(HEAD_DIM)] * 2 + [by_step((lines, half), lambda place, col=col: col) for col in (0, 1)] * 2
        + [by_step((out_lines, model_dim), lambda place: 0)] + [ANY] * 5,
        out_specs=[pl.BlockSpec((tile, BLOCK_LEN, rows), lambda t, d, place: (t, 0, d))] + [by_step((lines, half), lambda place: 1 - place[1])] * 4
        + [by_step((out_lines, model_dim), lambda place: 0, lambda place: (1 - place[1]) * steps)])
    square = jax.ShapeDtypeStruct((model_dim, model_dim), F32)
    return pl.pallas_call(
        kernel, grid_spec=grid_spec, name='input_grad', out_shape=[jax.ShapeDtypeStruct((n_seqs, BLOCK_LEN, model_dim), BF16)] + [square] * 5,
        input_output_aliases={14 + index: 1 + index for index in range(5)},
        cost_estimate=cost(4 * n_seqs * BLOCK_LEN * model_dim * width, 8 * n_seqs * BLOCK_LEN * width), compiler_params=params(TWO_LOOPS),
    )(place, d_proj, dp_mate, *weights, wb_mine, wb_mate, *[grad_mates[0]] * 2, *[grad_mates[1]] * 2, out_mate, *wholes, out_whole)


def weight_grads(core, x_all, d_proj, part):
    n_blocks, n_seqs, _, model_dim = x_all.shape
    half = model_dim // 2
    tile, rows = 16, 1024
    n_tiles = n_seqs // tile
    widths = (model_dim,) + (HEAD_DIM,) * part
    cols = (part, 2 * model_dim // HEAD_DIM)

    def kernel(core_ref, x_ref, *refs):
        sources, whole_refs, own_refs = refs[:len(widths)], refs[len(widths):len(widths) + 2], refs[len(widths) + 2:]

        @pl.when(pl.program_id(1) == 0)
        def _():
            for ref in own_refs:
                ref[...] = jnp.zeros_like(ref)

        for source, own_ref in zip(sources, own_refs):
            for at in range(0, source.shape[3], half):
                span = slice(at, min(at + half, source.shape[3]))
                own_ref[:, span] += mm_tn(flat(x_ref[0]), flat(source[0, :, :, span]))

        @pl.when(pl.program_id(1) == pl.num_programs(1) - 1)
        def _():
            for branch, ref in enumerate(whole_refs):
                ref[...] = own_refs[0][:, branch * half:(branch + 1) * half]

    def tokens(width, col_of):
        return pl.BlockSpec((1, tile, BLOCK_LEN, width), lambda d, t, core: (t // n_tiles, t % n_tiles, 0, col_of(d)))

    grid_spec = pltpu.PrefetchScalarGridSpec(
        num_scalar_prefetch=1, grid=(model_dim // rows, n_blocks * n_tiles),
        in_specs=[tokens(rows, lambda d: d)] + [tokens(width, lambda d, col=col: col) for width, col in zip(widths, cols)],
        out_specs=[pl.BlockSpec((rows, half), lambda d, t, core: (d, core[0]))] * 2 + [lead_spec((rows, width)) for width in widths])
    return pl.pallas_call(
        kernel, grid_spec=grid_spec, name='weight_grads',
        out_shape=[jax.ShapeDtypeStruct((model_dim, width), F32) for width in (model_dim, model_dim) + widths],
        cost_estimate=cost(x_all.size * 2 * model_dim, 8 * x_all.size), compiler_params=params(TWO_LOOPS),
    )(core, x_all, *[d_proj] * len(widths))


def out_weight_grad(core, hidden, dy_all):
    n_blocks, n_seqs, _, model_dim = dy_all.shape
    half = model_dim // 2
    tile, rows = 16, 1024
    n_tiles = n_seqs // tile

    def kernel(core_ref, h_ref, dy_ref, own_ref, whole_ref):
        @pl.when(pl.program_id(1) == 0)
        def _():
            own_ref[...] = jnp.zeros_like(own_ref)

        for at in range(0, model_dim, half):
            cols = slice(at, at + half)
            own_ref[:, cols] += mm_tn(flat(h_ref[0]), flat(dy_ref[0, :, :, cols]))

        @pl.when(pl.program_id(1) == pl.num_programs(1) - 1)
        def _():
            whole_ref[...] = own_ref[...]

    grid_spec = pltpu.PrefetchScalarGridSpec(
        num_scalar_prefetch=1, grid=(half // rows, n_blocks * n_tiles),
        in_specs=[pl.BlockSpec((1, tile, BLOCK_LEN, rows), lambda d, t, core: (t // n_tiles, t % n_tiles, 0, d)),
                  pl.BlockSpec((1, tile, BLOCK_LEN, model_dim), lambda d, t, core: (t // n_tiles, t % n_tiles, 0, 0))],
        out_specs=[lead_spec((rows, model_dim)),
                   pl.BlockSpec((rows, model_dim), lambda d, t, core: (d + core[0] * (half // rows), 0))])
    return pl.pallas_call(
        kernel, grid_spec=grid_spec, name='out_weight_grad',
        out_shape=[jax.ShapeDtypeStruct((half, model_dim), F32), jax.ShapeDtypeStruct((model_dim, model_dim), F32)],
        cost_estimate=cost(dy_all.size * model_dim, 4 * dy_all.size), compiler_params=params(TWO_LOOPS),
    )(core, hidden, dy_all)


def solution(mesh):
    n_sp = mesh.shape['sp']
    swap = [(rank, rank ^ 1) for rank in range(n_sp)]
    across = [(rank, rank ^ 2) for rank in range(n_sp)]

    def local_step(x_in, dy_out, w_query, w_key, w_value, w_beta, conv_query, conv_key, conv_value, w_gate, norm_weight, w_out):
        model_dim = x_in.shape[2]
        half = model_dim // 2
        half_heads = half // HEAD_DIM
        half_seqs = x_in.shape[0] // 2
        rank = lax.axis_index('sp')
        core = rank % 2
        mate = rank + 1 - 2 * core

        def my_cols(array_in, size=half, which=core):
            return lax.dynamic_slice_in_dim(array_in, which * size, size, axis=1)

        def swapped(array_in):
            return lax.ppermute(array_in, 'sp', swap)

        parts = (x_in[:half_seqs], x_in[half_seqs:])
        far_own = []
        for part in parts:
            far_own.append(lax.ppermute(part, 'sp', across))
        x_mate = swapped(x_in)
        squares = (w_query, w_key, w_value, w_gate)
        pad = ((0, 0), (0, HEAD_DIM - half_heads))
        wb_mine = jnp.pad(my_cols(w_beta, half_heads), pad)
        wb_mate = jnp.pad(my_cols(w_beta, half_heads, 1 - core), pad)
        half_taps = 0.5 * jnp.stack([my_cols(tap) for tap in (conv_key, conv_query, conv_value)]).astype(F32)
        norm = norm_weight.astype(F32).reshape(1, HEAD_DIM)
        core_s, mate_s = core.reshape(1), mate.reshape(1)
        place = jnp.stack([rank, core])

        def at_block(block):
            return jnp.stack([block, core])

        proj = project(at_block(rank), x_in, squares, wb_mine)
        proj = project(at_block(mate), x_mate, squares, wb_mine, 0, proj)
        begun = ()
        for index in range(2):
            far_mate = swapped(far_own[index])
            part = far_own[index]
            if begun:
                part, low = lax.optimization_barrier((part, begun[3]))
                begun = (*begun[:3], low, *begun[4:])
            first = index * half_seqs
            proj = project(at_block((rank + 2) % 4), part, squares, wb_mine, first, proj)
            proj = project(at_block((mate + 2) % 4), far_mate, squares, wb_mine, first, proj)
            begun = prep(proj, half_taps, half, first, half_seqs, begun)
        queries, keys, values, low, *convs = begun
        dy_all = lax.all_gather(dy_out, 'sp')
        x_all = lax.all_gather(x_in, 'sp')

        inverse = invert(low)
        hidden, hid_send, out, solved, states, inverse = delta_forward(mate_s, queries, keys, values, proj, norm, inverse)
        hid_mate = swapped(hid_send)
        d_hid = hidden_grad(core_s, dy_all, w_out)
        out_own, out_whole = out_weight_grad(core_s, hidden, dy_all)
        out_mate = swapped(out_own)
        y_out = output_dot(place, hidden, hid_mate, w_out)
        d_proj, dp_send, d_norm, d_taps = layer_backward(mate_s, d_hid, out, proj, (queries, keys, values), convs, norm, half_taps, solved, states, inverse)
        dp_mate = swapped(dp_send)
        small = jnp.concatenate([0.5 * jnp.sum(d_taps, axis=2).reshape(3 * CONV_TAPS, half), jnp.pad(jnp.sum(d_norm, axis=0, keepdims=True), ((0, 0), (0, half - HEAD_DIM)))])
        small_mate = swapped(small)

        wholes, dw_mate = [], []
        for part in range(2):
            *whole, dw_own, db_own = (*weight_grads(core_s, x_all, d_proj, part), None)[:4]
            wholes += whole
            dw_mate.append(swapped(dw_own))
        db_mate = swapped(db_own)
        dx_out, *dws = input_grad(place, d_proj, dp_mate, squares, wb_mine, wb_mate, dw_mate, out_mate, wholes, out_whole)

        def in_order(own_part, mate_part):
            return jnp.concatenate([jnp.where(core == 0, own_part, mate_part), jnp.where(core == 0, mate_part, own_part)], axis=1)

        dw_beta = in_order(db_own[:, :half_heads], db_mate[:, :half_heads])
        d_conv = in_order(small[:-1], small_mate[:-1]).reshape(3, CONV_TAPS, model_dim)
        norm_all = small[-1, :HEAD_DIM] + small_mate[-1, :HEAD_DIM]
        return (y_out, dx_out, dws[0], dws[1], dws[2], dw_beta, d_conv[1], d_conv[0], d_conv[2], dws[3], norm_all, dws[4])

    seq_part = P('dp', 'sp')
    full_mat = P()
    part_mat = P('dp')
    in_specs = (seq_part, seq_part) + (full_mat,) * 10
    out_specs = (seq_part, seq_part) + (part_mat,) * 10


    return jax.shard_map(local_step, mesh=mesh, in_specs=in_specs, out_specs=out_specs, check_vma=False)
```
